32 devices in a mesh: tiles: 2 (over x), rows: 8 (over z, y), dates: 2 (over core).
Axes of the slice: x: 2, y: 2, z: 4, core: 2. Of those that a mesh axis runs over, the one named last changes fastest.
Arguments:
- red_band: int32 [24, 512, 2048], P('dates', ('tiles', 'rows')), parts along dimension 1, may hold values from 1 to 1073741823
- nir_band: int32 [24, 512, 2048], P('dates', ('tiles', 'rows')), parts along dimension 1, may hold values from 1 to 1073741823
- cloud_class: int32 [24, 512, 2048], P('dates', ('tiles', 'rows')), parts along dimension 1, may hold values from 0 to 3
- date_ordinal: int32 [48], P(('tiles', 'dates')), parts along dimension 0, may hold values from 0 to 23, each once
Outputs:
- composite_red: int32 [512, 2048], P(('tiles', 'rows', 'dates')), parts along dimension 0
- composite_nir: int32 [512, 2048], P(('tiles', 'rows', 'dates')), parts along dimension 0
- chosen_date: int32 [512, 2048], P(('tiles', 'rows', 'dates')), parts along dimension 0
- overview_one: float32 [2, 256, 1024], P(None, ('tiles', 'rows', 'dates')), parts along dimension 1
- overview_two: float32 [2, 128, 512], P(None, ('tiles', 'rows', 'dates')), parts along dimension 1
- overview_three: float32 [2, 64, 256], P(None, ('tiles', 'rows', 'dates')), parts along dimension 1
The draws below stay inside these ranges and needn't reach their ends.
There are 2 independent parts, one for each index of `tiles`. The reference program is written for one: setup_inputs(seed, part) draws one part's arguments, and reference() takes and returns one part's arrays. A program takes and returns all parts, laid end to end along the dimension named above; each array names one. Nothing has to cross between parts.
Inputs may be any that keep to these rules, and one draw needn't show every extreme that they name: `date_ordinal`: each ordinal appears once.
All inputs are finite; a program needn't handle non-finite values.
Results may differ from the reference program's by a relative error of at most 0.0003.
Values sent between devices are 32-bit elements; how exact they have to be, the bound alone decides.
A program may use at most 192 MiB of HBM per device.

```python
import jax
import jax.numpy as jnp
from jax import lax

DATES = 24
W = 2048
LEVELS = 3
ROWS = 256


def draw_bands(key):
    base = jax.random.fold_in(key, 7101)
    keys = jax.random.split(base, 10)
    shape = (DATES, ROWS, W)
    plane = (ROWS, W)
    free_red = jax.random.randint(keys[0], shape, 1, 1073741824, dtype=jnp.int32)
    free_nir = jax.random.randint(keys[1], shape, 1, 1073741824, dtype=jnp.int32)
    kind = jax.random.randint(keys[2], plane, 0, 4, dtype=jnp.int32)[None]
    joined_code = jax.random.randint(keys[3], shape, 0, 16, dtype=jnp.int32)
    joined = joined_code % 2 == 1
    offset = joined_code // 2
    pair = jax.random.randint(keys[4], plane, 0, 4, dtype=jnp.int32)[None]
    table_red = jnp.where(pair == 2, 2, 1).astype(jnp.int32)
    table_nir = jnp.where(pair == 0, 39, jnp.where(pair == 1, 49, jnp.where(pair == 2, 97, 99))).astype(jnp.int32)
    factor = jax.random.randint(keys[5], shape, 1, 10737418, dtype=jnp.int32)
    near_red = jax.random.randint(keys[6], plane, 16777216, 33554432, dtype=jnp.int32)[None]
    near_nir = jax.random.randint(keys[7], plane, 1006632960, 1073741808, dtype=jnp.int32)[None]
    copy_red = jax.random.randint(keys[8], plane, 4194304, 8388608, dtype=jnp.int32)[None]
    copy_nir = jax.random.randint(keys[9], plane, 536870912, 1073741824, dtype=jnp.int32)[None]
    red = jnp.where(joined & (kind == 1), table_red * factor, free_red)
    nir = jnp.where(joined & (kind == 1), table_nir * factor + offset, free_nir)
    red = jnp.where(joined & (kind == 2), near_red + offset, red)
    nir = jnp.where(joined & (kind == 2), near_nir + offset, nir)
    red = jnp.where(joined & (kind == 3), copy_red + jnp.zeros(shape, jnp.int32), red)
    nir = jnp.where(joined & (kind == 3), copy_nir + jnp.zeros(shape, jnp.int32), nir)
    return (red.astype(jnp.int32), nir.astype(jnp.int32))


def draw_red_band(key, part):
    return draw_bands(key)[0]


def draw_nir_band(key, part):
    return draw_bands(key)[1]


def place_ends(drawn, rng, smallest, high):
    index_at = [jax.random.randint(jax.random.fold_in(rng, axis), (), 0, length) for axis, length in enumerate(drawn.shape)]
    longest = drawn.shape.index(max(drawn.shape))
    beside = index_at[:longest] + [(index_at[longest] + 1) % drawn.shape[longest]] + index_at[longest + 1:]
    return drawn.at[tuple(index_at)].set(smallest).at[tuple(beside)].set(high)


def setup_inputs(seed: int = 0, part: int = 0) -> dict:
    key_list = jax.random.split(jax.random.key(seed), 5)
    part_splits = jax.random.split(jax.random.fold_in(key_list[4], part), 5)
    red_band = draw_red_band(jax.random.fold_in(jax.random.fold_in(key_list[4], part), 71), part)
    nir_band = draw_nir_band(jax.random.fold_in(jax.random.fold_in(key_list[4], part), 71), part)
    cloud_class = place_ends(jax.random.randint(part_splits[2], (DATES, ROWS, W), 0, 4), jax.random.fold_in(part_splits[2], 1), 0, 3).astype(jnp.int32)
    date_ordinal = jax.random.permutation(part_splits[3], DATES).astype(jnp.int32)
    return dict(red_band=red_band, nir_band=nir_band, cloud_class=cloud_class, date_ordinal=date_ordinal)


KERNEL = (0.0625, 0.25, 0.375, 0.25, 0.0625)
LIMB = 32768
TWO_LIMBS = 1073741824
SCALE_BAND = 9.313225746154785e-10


def product_digits(small, large):
    small_hi = small // LIMB
    small_lo = small % LIMB
    large_top = large // TWO_LIMBS
    remain = large % TWO_LIMBS
    large_mid = remain // LIMB
    large_lo = remain % LIMB
    digit_zero = small_lo * large_lo
    digit_one = small_hi * large_lo + small_lo * large_mid
    digit_two = small_hi * large_mid + small_lo * large_top
    digit_three = small_hi * large_top
    digit_one = digit_one + digit_zero // LIMB
    digit_zero = digit_zero % LIMB
    digit_two = digit_two + digit_one // LIMB
    digit_one = digit_one % LIMB
    digit_three = digit_three + digit_two // LIMB
    digit_two = digit_two % LIMB
    return (digit_three, digit_two, digit_one, digit_zero)


def compare_digits(first, second):
    greater = first[0] > second[0]
    equal = first[0] == second[0]
    for one, two in zip(first[1:], second[1:]):
        greater = greater | (equal & (one > two))
        equal = equal & (one == two)
    return greater, equal


def better(first, second):
    clear_a, red_a, nir_a, ord_a = first
    clear_b, red_b, nir_b, ord_b = second
    diff_a = nir_a - red_a
    diff_b = nir_b - red_b
    total_a = nir_a + red_a
    total_b = nir_b + red_b
    sign_a = jnp.sign(diff_a)
    sign_b = jnp.sign(diff_b)
    greater, equal = compare_digits(product_digits(jnp.abs(diff_a), total_b), product_digits(jnp.abs(diff_b), total_a))
    lesser = jnp.logical_not(greater | equal)
    same_sign = sign_a == sign_b
    ndvi_more = (sign_a > sign_b) | (same_sign & (((sign_a > 0) & greater) | ((sign_a < 0) & lesser)))
    ndvi_same = same_sign & ((sign_a == 0) | equal)
    same_clear = clear_a == clear_b
    take = (clear_a > clear_b) | (same_clear & (ndvi_more | (ndvi_same & (ord_a < ord_b))))
    return tuple(jnp.where(take, one, two) for one, two in zip(first, second))


def blur_pool(level):
    rows = level.shape[1]
    cols = level.shape[2]
    padded = jnp.pad(level, ((0, 0), (2, 2), (0, 0)))
    smooth = KERNEL[0] * padded[:, 0:rows]
    for offset in range(1, 5):
        smooth = smooth + KERNEL[offset] * padded[:, offset:offset + rows]
    padded = jnp.pad(smooth, ((0, 0), (0, 0), (2, 2)))
    result = KERNEL[0] * padded[:, :, 0:cols]
    for offset in range(1, 5):
        result = result + KERNEL[offset] * padded[:, :, offset:offset + cols]
    return result.reshape(2, rows // 2, 2, cols // 2, 2).mean(axis=(2, 4))


def reference(red_band, nir_band, cloud_class, date_ordinal):
    def entry(index):
        return ((cloud_class[index] == 0).astype(jnp.int32), red_band[index], nir_band[index],
                jnp.full(red_band.shape[1:], date_ordinal[index], jnp.int32))

    def advance(carry, index):
        return better(carry, entry(index)), None

    best, unused = lax.scan(advance, entry(0), jnp.arange(1, DATES, dtype=jnp.int32))
    level = jnp.stack([best[1], best[2]]).astype(jnp.float32) * SCALE_BAND
    levels = []
    for number in range(LEVELS):
        level = blur_pool(level)
        levels.append(level)
    return best[1], best[2], best[3], levels[0], levels[1], levels[2]
```

```python
import functools

import jax
import jax.numpy as jnp
from jax import lax
from jax.experimental import pallas as pl
from jax.experimental.pallas import tpu as pltpu
from jax.sharding import PartitionSpec as P

LEVELS = 3
LIMB_BITS = 15
LIMB_MASK = (1 << LIMB_BITS) - 1
FLAG = 1 << 30
SCALE_BAND = 2.0**-30
LANES = 128
WIDTH = 256
MESH = pl.DeviceIdType.MESH


def taps(distance):
    far = (distance == 0) | (distance == 5)
    mid = (distance == 1) | (distance == 4)
    near = (distance == 2) | (distance == 3)
    return jnp.where(near, 0.3125, jnp.where(mid, 0.15625, jnp.where(far, 0.03125, 0.0)))


def limbs(value):
    return value >> LIMB_BITS, value & LIMB_MASK


def take_first(first, second):
    r1a, r0a, n1a, n0a, clear_a, ord_a = first
    r1b, r0b, n1b, n0b, clear_b, ord_b = second
    low = n0a * r0b - n0b * r0a + ((ord_b - ord_a) >> 31)
    mid = (n1a * r0b + n0a * r1b) - (n1b * r0a + n0b * r1a) + (low >> LIMB_BITS)
    high = n1a * r1b - n1b * r1a + (mid >> LIMB_BITS)
    return high + (clear_a - clear_b) >= 0


def pick(take, first, second):
    return tuple(jnp.where(take, one, two) for one, two in zip(first, second))


def joined(entry):
    r1, r0, n1, n0, clear, order = entry
    return (r1 << LIMB_BITS) | r0, (n1 << LIMB_BITS) | n0, clear, order


def dot_split(left, right, exact_left):
    data = right if exact_left else left
    high = data.astype(jnp.bfloat16)
    low = (data - high.astype(jnp.float32)).astype(jnp.bfloat16)
    if exact_left:
        dot = lambda part: jnp.dot(left, part, preferred_element_type=jnp.float32)
    else:
        dot = lambda part: jnp.dot(part, right, preferred_element_type=jnp.float32)
    return dot(high) + dot(low)


def filter_columns(source, weights):
    rows = source.shape[0]
    blocks = (source.shape[1] - 2 * LANES) // (2 * LANES)
    left = jnp.concatenate([source[:, 2 * LANES * b : 2 * LANES * b + 4 * LANES] for b in range(blocks)], axis=0)
    out = dot_split(left, weights, False)
    return [out[b * rows : (b + 1) * rows] for b in range(blocks)]


def iota(shape, axis):
    return lax.broadcasted_iota(jnp.int32, shape, axis)


def kernel(
    red, nir, cloud, ords, out_red, out_nir, out_ord, out_1, out_2, out_3,
    in_red, in_nir, in_cloud, best, arrived, wide_0, ybuf, wide_1, wide_2, zbuf,
    load_sem, send_sem, recv_sem,
):
    tile = lax.axis_index("tiles")
    strip_index = lax.axis_index("rows")
    core = lax.axis_index("dates")
    strips = lax.axis_size("rows")
    dates, strip, width = red.shape
    chunk = strip // 4
    half = width // 2
    has_outer = jnp.where(core == 0, strip_index > 0, strip_index < strips - 1)
    outer_strip = jnp.clip(strip_index + 2 * core - 1, 0, strips - 1)
    partner = (tile, strip_index, 1 - core)
    outer = (tile, outer_strip, 1 - core)
    rows_of = [(3 - 3 * core) * chunk, 3 * core * chunk, (2 - core) * chunk, (1 + core) * chunk]

    loads = []
    for slot, begin in enumerate(rows_of):
        begin = pl.multiple_of(begin, chunk)
        group = [
            pltpu.make_async_copy(
                source.at[:, pl.ds(begin, chunk), :], target.at[slot], load_sem.at[slot, number]
            )
            for number, (source, target) in enumerate(((red, in_red), (nir, in_nir), (cloud, in_cloud)))
        ]
        for copy in group:
            copy.start()
        loads.append(group)

    barrier = pltpu.get_barrier_semaphore()
    pl.semaphore_signal(barrier, inc=1, device_id=partner, device_id_type=MESH)

    @pl.when(has_outer)
    def _():
        pl.semaphore_signal(barrier, inc=1, device_id=outer, device_id_type=MESH)

    k = iota((4 * LANES, LANES), 0)
    j = iota((4 * LANES, LANES), 1)
    column_weights = taps(k - LANES - (2 * j - 2)).astype(jnp.bfloat16)

    @pl.when(jnp.logical_not(has_outer))
    def _():
        ybuf[3] = jnp.zeros(ybuf.shape[1:], jnp.float32)
        zbuf[2] = jnp.zeros(zbuf.shape[1:], jnp.float32)

    for wide in (wide_0, wide_1, wide_2):
        edge = jnp.zeros((wide.shape[0], LANES), jnp.float32)
        wide[:, 0:LANES] = edge
        wide[:, wide.shape[1] - LANES :] = edge

    def find_best(slot):
        for copy in loads[slot]:
            copy.wait()

        def step(number, unused):
            columns = pl.ds(pl.multiple_of(number * WIDTH, WIDTH), WIDTH)

            def entry(date):
                red_hi, red_lo = limbs(in_red[slot, date, :, columns])
                nir_hi, nir_lo = limbs(in_nir[slot, date, :, columns])
                clear = jnp.where(in_cloud[slot, date, :, columns] == 0, FLAG, 0)
                return (red_hi, red_lo, nir_hi, nir_lo, clear, jnp.full((chunk, WIDTH), ords[date], jnp.int32))

            current = entry(0)
            for date in range(1, dates):
                other = entry(date)
                current = pick(take_first(other, current), other, current)
            value_red, value_nir, clear, order = joined(current)
            best[slot, 0, :, columns] = value_red
            best[slot, 1, :, columns] = value_nir
            best[slot, 2, :, columns] = clear + order
            return unused

        lax.fori_loop(0, width // WIDTH, step, 0)

    def send_best(slot, place):
        copy = pltpu.make_async_remote_copy(
            src_ref=best.at[slot],
            dst_ref=arrived.at[place],
            send_sem=send_sem.at[place],
            recv_sem=recv_sem.at[place],
            device_id=partner,
            device_id_type=MESH,
        )
        copy.start()
        return copy

    def merge(slot, place, out_row):
        def step(number, unused):
            at = pl.multiple_of(number * WIDTH, WIDTH)
            columns = pl.ds(at, WIDTH)

            def entry(source):
                red_hi, red_lo = limbs(source[0, :, columns])
                nir_hi, nir_lo = limbs(source[1, :, columns])
                packed = source[2, :, columns]
                return (red_hi, red_lo, nir_hi, nir_lo, packed & FLAG, packed & (FLAG - 1))

            mine, theirs = entry(best.at[slot]), entry(arrived.at[place])
            value_red, value_nir, clear, order = joined(pick(take_first(theirs, mine), theirs, mine))
            if out_row is not None:
                rows = pl.ds(pl.multiple_of(out_row, chunk), chunk)
                out_red[rows, columns] = value_red
                out_nir[rows, columns] = value_nir
                out_ord[rows, columns] = order
            inner = pl.ds(pl.multiple_of(at + LANES, LANES), WIDTH)
            wide_0[0:chunk, inner] = value_red.astype(jnp.float32) * SCALE_BAND
            wide_0[chunk : 2 * chunk, inner] = value_nir.astype(jnp.float32) * SCALE_BAND
            return unused

        lax.fori_loop(0, width // WIDTH, step, 0)

    def columns_of(place):
        for number, block in enumerate(filter_columns(wide_0, column_weights)):
            ybuf[place, :, number * LANES : (number + 1) * LANES] = block

    find_best(0)
    pl.semaphore_wait(barrier, 1 + has_outer.astype(jnp.int32))
    send_0 = send_best(0, 0)
    find_best(1)
    send_0.wait_recv()
    merge(1, 0, core * chunk)
    columns_of(0)
    halo = pltpu.make_async_remote_copy(
        src_ref=ybuf.at[0],
        dst_ref=ybuf.at[3],
        send_sem=send_sem.at[3],
        recv_sem=recv_sem.at[3],
        device_id=outer,
        device_id_type=MESH,
    )

    @pl.when(has_outer)
    def _():
        halo.start()

    find_best(2)
    send_1 = send_best(2, 1)
    find_best(3)
    send_2 = send_best(3, 2)
    send_1.wait_recv()
    merge(3, 1, (1 - core) * chunk)
    columns_of(1)

    quarter = chunk // 2
    m = iota((4 * chunk, 8 * chunk), 0)
    band_m = m // (2 * chunk)
    within = m % (2 * chunk)
    row_1 = jnp.where(within < chunk, within, jnp.where(within < chunk + quarter, within - chunk - quarter, within - quarter))
    c = iota((4 * chunk, 8 * chunk), 1)
    place = c // (2 * chunk)
    band_c = (c // chunk) % 2
    from_core_0 = jnp.where(place == 3, -chunk, place * chunk)
    from_core_1 = chunk - from_core_0
    row_0 = jnp.where(core == 0, from_core_0, from_core_1) + c % chunk
    from_edge = jnp.where(core == 0, row_1, chunk - 1 - row_1)
    inside = from_edge >= jnp.where(has_outer, -chunk, 0)
    rows_1 = jnp.where((band_m == band_c) & inside, taps(row_0 - (2 * row_1 - 2)), 0.0)
    rows_1 = rows_1.astype(jnp.bfloat16)

    m = iota((3 * chunk, 4 * chunk), 0)
    packed = m >= 2 * chunk
    band_m = jnp.where(packed, (m - 2 * chunk) // quarter, m // chunk)
    row_2 = jnp.where(packed, m % quarter, m % chunk)
    c = iota((3 * chunk, 4 * chunk), 1)
    band_c = c // (2 * chunk)
    within = c % (2 * chunk)
    row_1 = jnp.where(within < chunk, within, jnp.where(within < chunk + quarter, within - chunk - quarter, within - quarter))
    rows_2 = jnp.where(band_m == band_c, taps(row_1 - (2 * row_2 - 2)), 0.0).astype(jnp.bfloat16)

    m = iota((2 * chunk, 3 * chunk), 0)
    c = iota((2 * chunk, 3 * chunk), 1)
    place = c // chunk
    toward = quarter * (1 - 2 * core)
    side = jnp.where(place == 0, 0, jnp.where(place == 1, toward, -toward))
    row_2 = c % quarter + side
    rows_3 = jnp.where(m // chunk == (c % chunk) // quarter, taps(row_2 - (2 * (m % chunk) - 2)), 0.0)
    rows_3 = rows_3.astype(jnp.bfloat16)

    send_2.wait_recv()
    merge(2, 2, None)
    columns_of(2)

    @pl.when(has_outer)
    def _():
        halo.wait_recv()

    level_1 = dot_split(rows_1, ybuf[...].reshape(8 * chunk, half), True)
    wide_1[:, LANES : LANES + half] = level_1
    out_1[0] = level_1[0:chunk]
    out_1[1] = level_1[2 * chunk : 3 * chunk]
    data = jnp.concatenate(filter_columns(wide_1, column_weights), axis=1)
    level_2 = dot_split(rows_2, data, True)
    wide_2[:, LANES : LANES + half // 2] = level_2[2 * chunk :]
    out_2[0] = level_2[0:quarter]
    out_2[1] = level_2[chunk : chunk + quarter]
    zbuf[0] = jnp.concatenate(filter_columns(wide_2, column_weights), axis=1)

    def send_z(slot, device):
        return pltpu.make_async_remote_copy(
            src_ref=zbuf.at[0],
            dst_ref=zbuf.at[slot],
            send_sem=send_sem.at[3 + slot],
            recv_sem=recv_sem.at[3 + slot],
            device_id=device,
            device_id_type=MESH,
        )

    to_partner, to_outer = send_z(1, partner), send_z(2, outer)

    @pl.when(has_outer)
    def _():
        to_outer.start()

    to_partner.start()
    to_partner.wait_recv()

    @pl.when(has_outer)
    def _():
        to_outer.wait_recv()

    level_3 = dot_split(rows_3, zbuf[...].reshape(3 * chunk, zbuf.shape[2]), True)
    out_3[0] = level_3[0 : quarter // 2]
    out_3[1] = level_3[chunk : chunk + quarter // 2]

    for copy in (send_0, send_1, send_2, to_partner):
        copy.wait_send()

    @pl.when(has_outer)
    def _():
        halo.wait_send()
        to_outer.wait_send()


def body(red_band, nir_band, cloud_class, date_ordinal):
    dates, strip, width = red_band.shape
    own = strip // 2
    chunk = strip // 4
    whole = pl.BlockSpec(memory_space=pltpu.VMEM)
    anywhere = pl.BlockSpec(memory_space=pl.ANY)
    outs = [jax.ShapeDtypeStruct((own, width), jnp.int32)] * 3
    outs += [jax.ShapeDtypeStruct((2, own >> n, width >> n), jnp.float32) for n in range(1, LEVELS + 1)]
    stream = pltpu.VMEM((4, dates, chunk, width), jnp.int32)
    return pl.pallas_call(
        kernel,
        out_shape=outs,
        in_specs=[anywhere] * 3 + [pl.BlockSpec(memory_space=pltpu.SMEM)],
        out_specs=[whole] * 6,
        scratch_shapes=[
            stream,
            stream,
            stream,
            pltpu.VMEM((4, 3, chunk, width), jnp.int32),
            pltpu.VMEM((3, 3, chunk, width), jnp.int32),
            pltpu.VMEM((2 * chunk, width + 2 * LANES), jnp.float32),
            pltpu.VMEM((4, 2 * chunk, width // 2), jnp.float32),
            pltpu.VMEM((4 * chunk, width // 2 + 2 * LANES), jnp.float32),
            pltpu.VMEM((chunk, width // 4 + 2 * LANES), jnp.float32),
            pltpu.VMEM((3, chunk, width // 8), jnp.float32),
            pltpu.SemaphoreType.DMA((4, 3)),
            pltpu.SemaphoreType.DMA((6,)),
            pltpu.SemaphoreType.DMA((6,)),
        ],
        compiler_params=pltpu.CompilerParams(collective_id=0, has_side_effects=True),
        name="composite",
    )(red_band, nir_band, cloud_class, date_ordinal)


def solution(mesh):
    in_specs = (
        P("dates", ("tiles", "rows"), None),
        P("dates", ("tiles", "rows"), None),
        P("dates", ("tiles", "rows"), None),
        P(("tiles", "dates")),
    )
    out_specs = (
        P(("tiles", "rows", "dates"), None),
        P(("tiles", "rows", "dates"), None),
        P(("tiles", "rows", "dates"), None),
        P(None, ("tiles", "rows", "dates"), None),
        P(None, ("tiles", "rows", "dates"), None),
        P(None, ("tiles", "rows", "dates"), None),
    )
    return jax.shard_map(body, mesh=mesh, in_specs=in_specs, out_specs=out_specs, check_vma=False)
```

```python
import functools

import jax
import jax.numpy as jnp
from jax import lax
from jax.experimental import pallas as pl
from jax.experimental.pallas import tpu as pltpu
from jax.sharding import PartitionSpec as P

LEVELS = 3
LIMB_BITS = 15
LIMB_MASK = (1 << LIMB_BITS) - 1
FLAG = 1 << 30
SCALE_BAND = 2.0**-30
LANES = 128
WIDTH = 256
MESH = pl.DeviceIdType.MESH


def taps(distance):
    far = (distance == 0) | (distance == 5)
    mid = (distance == 1) | (distance == 4)
    near = (distance == 2) | (distance == 3)
    return jnp.where(near, 0.3125, jnp.where(mid, 0.15625, jnp.where(far, 0.03125, 0.0)))


def limbs(value):
    return value >> LIMB_BITS, value & LIMB_MASK


def take_first(first, second):
    r1a, r0a, n1a, n0a, clear_a, ord_a = first
    r1b, r0b, n1b, n0b, clear_b, ord_b = second
    low = n0a * r0b - n0b * r0a + ((ord_b - ord_a) >> 31)
    mid = (n1a * r0b + n0a * r1b) - (n1b * r0a + n0b * r1a) + (low >> LIMB_BITS)
    high = n1a * r1b - n1b * r1a + (mid >> LIMB_BITS)
    return high + (clear_a - clear_b) >= 0


def pick(take, first, second):
    return tuple(jnp.where(take, one, two) for one, two in zip(first, second))


def joined(entry):
    r1, r0, n1, n0, clear, order = entry
    return (r1 << LIMB_BITS) | r0, (n1 << LIMB_BITS) | n0, clear, order


def dot_split(left, right, exact_left):
    data = right if exact_left else left
    high = data.astype(jnp.bfloat16)
    low = (data - high.astype(jnp.float32)).astype(jnp.bfloat16)
    if exact_left:
        dot = lambda part: jnp.dot(left, part, preferred_element_type=jnp.float32)
    else:
        dot = lambda part: jnp.dot(part, right, preferred_element_type=jnp.float32)
    return dot(high) + dot(low)


def filter_columns(source, weights):
    rows = source.shape[0]
    blocks = (source.shape[1] - 2 * LANES) // (2 * LANES)
    left = jnp.concatenate([source[:, 2 * LANES * b : 2 * LANES * b + 4 * LANES] for b in range(blocks)], axis=0)
    out = dot_split(left, weights, False)
    return [out[b * rows : (b + 1) * rows] for b in range(blocks)]


def iota(shape, axis):
    return lax.broadcasted_iota(jnp.int32, shape, axis)


def kernel(
    red, nir, cloud, ords, out_red, out_nir, out_ord, out_1, out_2, out_3,
    in_red, in_nir, in_cloud, best, arrived, wide_0, ybuf, wide_1, wide_2, zbuf,
    load_sem, send_sem, recv_sem,
):
    tile = lax.axis_index("tiles")
    strip_index = lax.axis_index("rows")
    core = lax.axis_index("dates")
    strips = lax.axis_size("rows")
    dates, strip, width = red.shape
    chunk = strip // 4
    half = width // 2
    has_outer = jnp.where(core == 0, strip_index > 0, strip_index < strips - 1)
    outer_strip = jnp.clip(strip_index + 2 * core - 1, 0, strips - 1)
    partner = (tile, strip_index, 1 - core)
    outer = (tile, outer_strip, 1 - core)
    rows_of = [(3 - 3 * core) * chunk, 3 * core * chunk, (2 - core) * chunk, (1 + core) * chunk]

    loads = []
    for slot, begin in enumerate(rows_of):
        begin = pl.multiple_of(begin, chunk)
        group = [
            pltpu.make_async_copy(
                source.at[:, pl.ds(begin, chunk), :], target.at[slot], load_sem.at[slot, number]
            )
            for number, (source, target) in enumerate(((red, in_red), (nir, in_nir), (cloud, in_cloud)))
        ]
        for copy in group:
            copy.start()
        loads.append(group)

    barrier = pltpu.get_barrier_semaphore()
    pl.semaphore_signal(barrier, inc=1, device_id=partner, device_id_type=MESH)

    @pl.when(has_outer)
    def _():
        pl.semaphore_signal(barrier, inc=1, device_id=outer, device_id_type=MESH)

    k = iota((4 * LANES, LANES), 0)
    j = iota((4 * LANES, LANES), 1)
    column_weights = taps(k - LANES - (2 * j - 2)).astype(jnp.bfloat16)

    @pl.when(jnp.logical_not(has_outer))
    def _():
        ybuf[3] = jnp.zeros(ybuf.shape[1:], jnp.float32)
        zbuf[2] = jnp.zeros(zbuf.shape[1:], jnp.float32)

    for wide in (wide_0, wide_1, wide_2):
        edge = jnp.zeros((wide.shape[0], LANES), jnp.float32)
        wide[:, 0:LANES] = edge
        wide[:, wide.shape[1] - LANES :] = edge

    def find_best(slot):
        for copy in loads[slot]:
            copy.wait()

        def step(number, unused):
            columns = pl.ds(pl.multiple_of(number * WIDTH, WIDTH), WIDTH)

            def entry(date):
                red_hi, red_lo = limbs(in_red[slot, date, :, columns])
                nir_hi, nir_lo = limbs(in_nir[slot, date, :, columns])
                clear = jnp.where(in_cloud[slot, date, :, columns] == 0, FLAG, 0)
                return (red_hi, red_lo, nir_hi, nir_lo, clear, jnp.full((chunk, WIDTH), ords[date], jnp.int32))

            current = entry(0)
            for date in range(1, dates):
                other = entry(date)
                current = pick(take_first(other, current), other, current)
            value_red, value_nir, clear, order = joined(current)
            best[slot, 0, :, columns] = value_red
            best[slot, 1, :, columns] = value_nir
            best[slot, 2, :, columns] = clear + order
            return unused

        lax.fori_loop(0, width // WIDTH, step, 0)

    def send_best(slot, place):
        copy = pltpu.make_async_remote_copy(
            src_ref=best.at[slot],
            dst_ref=arrived.at[place],
            send_sem=send_sem.at[place],
            recv_sem=recv_sem.at[place],
            device_id=partner,
            device_id_type=MESH,
        )
        copy.start()
        return copy

    def merge(slot, place, out_row):
        def step(number, unused):
            at = pl.multiple_of(number * WIDTH, WIDTH)
            columns = pl.ds(at, WIDTH)

            def entry(source):
                red_hi, red_lo = limbs(source[0, :, columns])
                nir_hi, nir_lo = limbs(source[1, :, columns])
                packed = source[2, :, columns]
                return (red_hi, red_lo, nir_hi, nir_lo, packed & FLAG, packed & (FLAG - 1))

            mine, theirs = entry(best.at[slot]), entry(arrived.at[place])
            value_red, value_nir, clear, order = joined(pick(take_first(theirs, mine), theirs, mine))
            if out_row is not None:
                rows = pl.ds(pl.multiple_of(out_row, chunk), chunk)
                out_red[rows, columns] = value_red
                out_nir[rows, columns] = value_nir
                out_ord[rows, columns] = order
            inner = pl.ds(pl.multiple_of(at + LANES, LANES), WIDTH)
            wide_0[0:chunk, inner] = value_red.astype(jnp.float32) * SCALE_BAND
            wide_0[chunk : 2 * chunk, inner] = value_nir.astype(jnp.float32) * SCALE_BAND
            return unused

        lax.fori_loop(0, width // WIDTH, step, 0)

    def columns_of(place):
        for number, block in enumerate(filter_columns(wide_0, column_weights)):
            ybuf[place, :, number * LANES : (number + 1) * LANES] = block

    find_best(0)
    pl.semaphore_wait(barrier, 1 + has_outer.astype(jnp.int32))
    send_0 = send_best(0, 0)
    find_best(1)
    send_0.wait_recv()
    merge(1, 0, core * chunk)
    columns_of(0)
    halo = pltpu.make_async_remote_copy(
        src_ref=ybuf.at[0],
        dst_ref=ybuf.at[3],
        send_sem=send_sem.at[3],
        recv_sem=recv_sem.at[3],
        device_id=outer,
        device_id_type=MESH,
    )

    @pl.when(has_outer)
    def _():
        halo.start()

    find_best(2)
    send_1 = send_best(2, 1)
    find_best(3)
    send_2 = send_best(3, 2)
    send_1.wait_recv()
    merge(3, 1, (1 - core) * chunk)
    columns_of(1)

    quarter = chunk // 2
    m = iota((4 * chunk, 8 * chunk), 0)
    band_m = m // (2 * chunk)
    within = m % (2 * chunk)
    row_1 = jnp.where(within < chunk, within, jnp.where(within < chunk + quarter, within - chunk - quarter, within - quarter))
    c = iota((4 * chunk, 8 * chunk), 1)
    place = c // (2 * chunk)
    band_c = (c // chunk) % 2
    from_core_0 = jnp.where(place == 3, -chunk, place * chunk)
    from_core_1 = chunk - from_core_0
    row_0 = jnp.where(core == 0, from_core_0, from_core_1) + c % chunk
    from_edge = jnp.where(core == 0, row_1, chunk - 1 - row_1)
    inside = from_edge >= jnp.where(has_outer, -chunk, 0)
    rows_1 = jnp.where((band_m == band_c) & inside, taps(row_0 - (2 * row_1 - 2)), 0.0)
    rows_1 = rows_1.astype(jnp.bfloat16)

    m = iota((3 * chunk, 4 * chunk), 0)
    packed = m >= 2 * chunk
    band_m = jnp.where(packed, (m - 2 * chunk) // quarter, m // chunk)
    row_2 = jnp.where(packed, m % quarter, m % chunk)
    c = iota((3 * chunk, 4 * chunk), 1)
    band_c = c // (2 * chunk)
    within = c % (2 * chunk)
    row_1 = jnp.where(within < chunk, within, jnp.where(within < chunk + quarter, within - chunk - quarter, within - quarter))
    rows_2 = jnp.where(band_m == band_c, taps(row_1 - (2 * row_2 - 2)), 0.0).astype(jnp.bfloat16)

    m = iota((2 * chunk, 3 * chunk), 0)
    c = iota((2 * chunk, 3 * chunk), 1)
    place = c // chunk
    toward = quarter * (1 - 2 * core)
    side = jnp.where(place == 0, 0, jnp.where(place == 1, toward, -toward))
    row_2 = c % quarter + side
    rows_3 = jnp.where(m // chunk == (c % chunk) // quarter, taps(row_2 - (2 * (m % chunk) - 2)), 0.0)
    rows_3 = rows_3.astype(jnp.bfloat16)

    send_2.wait_recv()
    merge(2, 2, None)
    columns_of(2)

    @pl.when(has_outer)
    def _():
        halo.wait_recv()

    level_1 = dot_split(rows_1, ybuf[...].reshape(8 * chunk, half), True)
    wide_1[:, LANES : LANES + half] = level_1
    out_1[0] = level_1[0:chunk]
    out_1[1] = level_1[2 * chunk : 3 * chunk]
    data = jnp.concatenate(filter_columns(wide_1, column_weights), axis=1)
    level_2 = dot_split(rows_2, data, True)
    wide_2[:, LANES : LANES + half // 2] = level_2[2 * chunk :]
    out_2[0] = level_2[0:quarter]
    out_2[1] = level_2[chunk : chunk + quarter]
    zbuf[0] = jnp.concatenate(filter_columns(wide_2, column_weights), axis=1)

    def send_z(slot, device):
        return pltpu.make_async_remote_copy(
            src_ref=zbuf.at[0],
            dst_ref=zbuf.at[slot],
            send_sem=send_sem.at[3 + slot],
            recv_sem=recv_sem.at[3 + slot],
            device_id=device,
            device_id_type=MESH,
        )

    to_partner, to_outer = send_z(1, partner), send_z(2, outer)

    @pl.when(has_outer)
    def _():
        to_outer.start()

    to_partner.start()
    to_partner.wait_recv()

    @pl.when(has_outer)
    def _():
        to_outer.wait_recv()

    level_3 = dot_split(rows_3, zbuf[...].reshape(3 * chunk, zbuf.shape[2]), True)
    out_3[0] = level_3[0 : quarter // 2]
    out_3[1] = level_3[chunk : chunk + quarter // 2]

    for copy in (send_0, send_1, send_2, to_partner):
        copy.wait_send()

    @pl.when(has_outer)
    def _():
        halo.wait_send()
        to_outer.wait_send()


def write_out(*refs):
    count = len(refs) // 2
    semaphores = refs[-1]
    copies = [pltpu.make_async_copy(refs[n], refs[count + n], semaphores.at[n]) for n in range(count)]
    for copy in copies:
        copy.start()
    for copy in copies:
        copy.wait()


def body(red_band, nir_band, cloud_class, date_ordinal):
    dates, strip, width = red_band.shape
    own = strip // 2
    chunk = strip // 4
    whole = pl.BlockSpec(memory_space=pltpu.VMEM)
    anywhere = pl.BlockSpec(memory_space=pl.ANY)
    outs = [jax.ShapeDtypeStruct((own, width), jnp.int32)] * 3
    outs += [jax.ShapeDtypeStruct((2, own >> n, width >> n), jnp.float32) for n in range(1, LEVELS + 1)]
    kept = [pltpu.VMEM(out.shape, out.dtype) for out in outs]
    stream = pltpu.VMEM((4, dates, chunk, width), jnp.int32)
    results = pl.pallas_call(
        kernel,
        out_shape=kept,
        in_specs=[anywhere] * 3 + [pl.BlockSpec(memory_space=pltpu.SMEM)],
        out_specs=[whole] * 6,
        scratch_shapes=[
            stream,
            stream,
            stream,
            pltpu.VMEM((4, 3, chunk, width), jnp.int32),
            pltpu.VMEM((3, 3, chunk, width), jnp.int32),
            pltpu.VMEM((2 * chunk, width + 2 * LANES), jnp.float32),
            pltpu.VMEM((4, 2 * chunk, width // 2), jnp.float32),
            pltpu.VMEM((4 * chunk, width // 2 + 2 * LANES), jnp.float32),
            pltpu.VMEM((chunk, width // 4 + 2 * LANES), jnp.float32),
            pltpu.VMEM((3, chunk, width // 8), jnp.float32),
            pltpu.SemaphoreType.DMA((4, 3)),
            pltpu.SemaphoreType.DMA((6,)),
            pltpu.SemaphoreType.DMA((6,)),
        ],
        compiler_params=pltpu.CompilerParams(collective_id=0, has_side_effects=True),
        name="composite",
    )(red_band, nir_band, cloud_class, date_ordinal)
    return pl.pallas_call(
        write_out,
        out_shape=outs,
        in_specs=[whole] * 6,
        out_specs=[anywhere] * 6,
        scratch_shapes=[pltpu.SemaphoreType.DMA((6,))],
        name="write_out",
    )(*[pltpu.with_memory_space_constraint(result, pltpu.VMEM) for result in results])


def solution(mesh):
    in_specs = (
        P("dates", ("tiles", "rows"), None),
        P("dates", ("tiles", "rows"), None),
        P("dates", ("tiles", "rows"), None),
        P(("tiles", "dates")),
    )
    out_specs = (
        P(("tiles", "rows", "dates"), None),
        P(("tiles", "rows", "dates"), None),
        P(("tiles", "rows", "dates"), None),
        P(None, ("tiles", "rows", "dates"), None),
        P(None, ("tiles", "rows", "dates"), None),
        P(None, ("tiles", "rows", "dates"), None),
    )
    return jax.shard_map(body, mesh=mesh, in_specs=in_specs, out_specs=out_specs, check_vma=False)
```

```python
import functools

import jax
import jax.numpy as jnp
from jax import lax
from jax.experimental import pallas as pl
from jax.experimental.pallas import tpu as pltpu
from jax.sharding import PartitionSpec as P

LEVELS = 3
LIMB_BITS = 15
LIMB_MASK = (1 << LIMB_BITS) - 1
FLAG = 1 << 30
SCALE_BAND = 2.0**-30
LANES = 128
WIDTH = 512
PARTS = 2
MESH = pl.DeviceIdType.MESH


def taps(distance):
    far = (distance == 0) | (distance == 5)
    mid = (distance == 1) | (distance == 4)
    near = (distance == 2) | (distance == 3)
    return jnp.where(near, 0.3125, jnp.where(mid, 0.15625, jnp.where(far, 0.03125, 0.0)))


def limbs(value):
    return value >> LIMB_BITS, value & LIMB_MASK


def take_first(first, second):
    r1a, r0a, n1a, n0a, clear_a, ord_a = first
    r1b, r0b, n1b, n0b, clear_b, ord_b = second
    low = n0a * r0b - n0b * r0a + ((ord_b - ord_a) >> 31)
    mid = (n1a * r0b + n0a * r1b) - (n1b * r0a + n0b * r1a) + (low >> LIMB_BITS)
    high = n1a * r1b - n1b * r1a + (mid >> LIMB_BITS)
    return high >= clear_b - clear_a


def pick(take, first, second):
    return tuple(jnp.where(take, one, two) for one, two in zip(first, second))


def joined(entry):
    r1, r0, n1, n0, clear, order = entry
    return (r1 << LIMB_BITS) | r0, (n1 << LIMB_BITS) | n0, clear, order


def dot_split(left, right, exact_left):
    data = right if exact_left else left
    high = data.astype(jnp.bfloat16)
    low = (data - high.astype(jnp.float32)).astype(jnp.bfloat16)
    if exact_left:
        dot = lambda part: jnp.dot(left, part, preferred_element_type=jnp.float32)
    else:
        dot = lambda part: jnp.dot(part, right, preferred_element_type=jnp.float32)
    return dot(high) + dot(low)


def filter_columns(source, weights):
    rows = source.shape[0]
    blocks = (source.shape[1] - 2 * LANES) // (2 * LANES)
    left = jnp.concatenate([source[:, 2 * LANES * b : 2 * LANES * b + 4 * LANES] for b in range(blocks)], axis=0)
    out = dot_split(left, weights, False)
    return [out[b * rows : (b + 1) * rows] for b in range(blocks)]


def iota(shape, axis):
    return lax.broadcasted_iota(jnp.int32, shape, axis)


def kernel(
    red, nir, cloud, ordinals, out_red, out_nir, out_ord, out_1, out_2, out_3,
    in_red, in_nir, in_cloud, best, arrived, wide_0, ybuf, wide_1, wide_2, zbuf,
    ords, load_sem, order_sem, send_sem, recv_sem,
):
    tile = lax.axis_index("tiles")
    strip_index = lax.axis_index("rows")
    core = lax.axis_index("dates")
    strips = lax.axis_size("rows")
    dates, strip, width = red.shape
    chunk = strip // 4
    half = width // 2
    has_outer = jnp.where(core == 0, strip_index > 0, strip_index < strips - 1)
    outer_strip = jnp.clip(strip_index + 2 * core - 1, 0, strips - 1)
    partner = (tile, strip_index, 1 - core)
    outer = (tile, outer_strip, 1 - core)
    rows_of = [(3 - 3 * core) * chunk, 3 * core * chunk, (2 - core) * chunk, (1 + core) * chunk]

    loads = []
    piece = width // PARTS
    for slot, begin in enumerate(rows_of):
        begin = pl.multiple_of(begin, chunk)
        for part in range(PARTS):
            columns = pl.ds(part * piece, piece)
            group = [
                pltpu.make_async_copy(
                    source.at[:, pl.ds(begin, chunk), columns],
                    target.at[slot, :, :, columns],
                    load_sem.at[slot, part, number],
                )
                for number, (source, target) in enumerate(((red, in_red), (nir, in_nir), (cloud, in_cloud)))
            ]
            for copy in group:
                copy.start()
            loads.append(group)
    order_copy = pltpu.make_async_copy(ordinals, ords, order_sem)
    order_copy.start()

    barrier = pltpu.get_barrier_semaphore()
    pl.semaphore_signal(barrier, inc=1, device_id=partner, device_id_type=MESH)

    @pl.when(has_outer)
    def _():
        pl.semaphore_signal(barrier, inc=1, device_id=outer, device_id_type=MESH)

    k = iota((4 * LANES, LANES), 0)
    j = iota((4 * LANES, LANES), 1)
    column_weights = taps(k - LANES - (2 * j - 2)).astype(jnp.bfloat16)

    @pl.when(jnp.logical_not(has_outer))
    def _():
        ybuf[2] = jnp.zeros(ybuf.shape[1:], jnp.float32)
        zbuf[2] = jnp.zeros(zbuf.shape[1:], jnp.float32)

    for wide in (wide_0, wide_1, wide_2):
        edge = jnp.zeros((wide.shape[0], LANES), jnp.float32)
        wide[:, 0:LANES] = edge
        wide[:, wide.shape[1] - LANES :] = edge

    order_copy.wait()

    def find_best(slot, part):
        for copy in loads[slot * PARTS + part]:
            copy.wait()

        def step(number, unused):
            columns = pl.ds(pl.multiple_of(number * WIDTH + part * piece, WIDTH), WIDTH)

            def entry(date):
                red_hi, red_lo = limbs(in_red[slot, date, :, columns])
                nir_hi, nir_lo = limbs(in_nir[slot, date, :, columns])
                clear = jnp.where(in_cloud[slot, date, :, columns] == 0, FLAG, 0)
                return (red_hi, red_lo, nir_hi, nir_lo, clear, jnp.full((chunk, WIDTH), ords[date], jnp.int32))

            current = entry(0)
            for date in range(1, dates):
                other = entry(date)
                current = pick(take_first(other, current), other, current)
            value_red, value_nir, clear, order = joined(current)
            best[slot, 0, :, columns] = value_red
            best[slot, 1, :, columns] = value_nir
            best[slot, 2, :, columns] = clear + order
            return unused

        lax.fori_loop(0, piece // WIDTH, step, 0)

    partner_sends = []

    def send_best(slot, place, part):
        columns = pl.ds(part * piece, piece)
        copy = pltpu.make_async_remote_copy(
            src_ref=best.at[slot, :, :, columns],
            dst_ref=arrived.at[place, :, :, columns],
            send_sem=send_sem.at[3 + place * PARTS + part],
            recv_sem=recv_sem.at[3 + place * PARTS + part],
            device_id=partner,
            device_id_type=MESH,
        )
        copy.start()
        partner_sends.append(copy)

    def wait_best(place):
        for copy in partner_sends[place * PARTS : (place + 1) * PARTS]:
            copy.wait_recv()

    def merge(slot, place, out_row):
        def step(number, unused):
            at = pl.multiple_of(number * WIDTH, WIDTH)
            columns = pl.ds(at, WIDTH)

            def entry(source):
                red_hi, red_lo = limbs(source[0, :, columns])
                nir_hi, nir_lo = limbs(source[1, :, columns])
                packed = source[2, :, columns]
                return (red_hi, red_lo, nir_hi, nir_lo, packed & FLAG, packed & (FLAG - 1))

            mine, theirs = entry(best.at[slot]), entry(arrived.at[place])
            value_red, value_nir, clear, order = joined(pick(take_first(theirs, mine), theirs, mine))
            if out_row is not None:
                rows = pl.ds(pl.multiple_of(out_row, chunk), chunk)
                out_red[rows, columns] = value_red
                out_nir[rows, columns] = value_nir
                out_ord[rows, columns] = order
            inner = pl.ds(pl.multiple_of(at + LANES, LANES), WIDTH)
            wide_0[0:chunk, inner] = value_red.astype(jnp.float32) * SCALE_BAND
            wide_0[chunk : 2 * chunk, inner] = value_nir.astype(jnp.float32) * SCALE_BAND
            return unused

        lax.fori_loop(0, width // WIDTH, step, 0)

    def columns_of(place):
        for number, block in enumerate(filter_columns(wide_0, column_weights)):
            ybuf[place, :, number * LANES : (number + 1) * LANES] = block

    for part in range(PARTS):
        find_best(0, part)
        if part == 0:
            pl.semaphore_wait(barrier, 1 + has_outer.astype(jnp.int32))
        send_best(0, 0, part)
    for part in range(PARTS):
        find_best(1, part)
    wait_best(0)
    merge(1, 0, core * chunk)
    columns_of(0)
    halo = pltpu.make_async_remote_copy(
        src_ref=ybuf.at[0],
        dst_ref=ybuf.at[2],
        send_sem=send_sem.at[0],
        recv_sem=recv_sem.at[0],
        device_id=outer,
        device_id_type=MESH,
    )

    @pl.when(has_outer)
    def _():
        halo.start()

    for slot, place in ((2, 1), (3, 2)):
        for part in range(PARTS):
            find_best(slot, part)
            send_best(slot, place, part)
    wait_best(1)
    merge(3, 1, (1 - core) * chunk)
    columns_of(1)

    quarter = chunk // 2
    def row_weights(first, count):
        shape = (4 * chunk, count * 2 * chunk)
        m = iota(shape, 0)
        band_m = m // (2 * chunk)
        within = m % (2 * chunk)
        row_1 = jnp.where(within < chunk, within, jnp.where(within < chunk + quarter, within - chunk - quarter, within - quarter))
        c = iota(shape, 1)
        place = c // (2 * chunk) + first
        band_c = (c // chunk) % 2
        from_core_0 = jnp.where(place == 2, -chunk, jnp.where(place == 3, 2 * chunk, place * chunk))
        from_core_1 = chunk - from_core_0
        row_0 = jnp.where(core == 0, from_core_0, from_core_1) + c % chunk
        from_edge = jnp.where(core == 0, row_1, chunk - 1 - row_1)
        inside = from_edge >= jnp.where(has_outer, -chunk, 0)
        return jnp.where((band_m == band_c) & inside, taps(row_0 - (2 * row_1 - 2)), 0.0).astype(jnp.bfloat16)

    rows_1a, rows_1b = row_weights(0, 3), row_weights(3, 1)

    m = iota((3 * chunk, 4 * chunk), 0)
    packed = m >= 2 * chunk
    band_m = jnp.where(packed, (m - 2 * chunk) // quarter, m // chunk)
    row_2 = jnp.where(packed, m % quarter, m % chunk)
    c = iota((3 * chunk, 4 * chunk), 1)
    band_c = c // (2 * chunk)
    within = c % (2 * chunk)
    row_1 = jnp.where(within < chunk, within, jnp.where(within < chunk + quarter, within - chunk - quarter, within - quarter))
    rows_2 = jnp.where(band_m == band_c, taps(row_1 - (2 * row_2 - 2)), 0.0).astype(jnp.bfloat16)

    m = iota((2 * chunk, 3 * chunk), 0)
    c = iota((2 * chunk, 3 * chunk), 1)
    place = c // chunk
    toward = quarter * (1 - 2 * core)
    side = jnp.where(place == 0, 0, jnp.where(place == 1, toward, -toward))
    row_2 = c % quarter + side
    rows_3 = jnp.where(m // chunk == (c % chunk) // quarter, taps(row_2 - (2 * (m % chunk) - 2)), 0.0)
    rows_3 = rows_3.astype(jnp.bfloat16)

    def next_levels(level_1):
        wide_1[:, LANES : LANES + half] = level_1
        data = jnp.concatenate(filter_columns(wide_1, column_weights), axis=1)
        level_2 = dot_split(rows_2, data, True)
        wide_2[:, LANES : LANES + half // 2] = level_2[2 * chunk :]
        return level_2, jnp.concatenate(filter_columns(wide_2, column_weights), axis=1)

    def send_z(source, slot, device):
        return pltpu.make_async_remote_copy(
            src_ref=zbuf.at[source],
            dst_ref=zbuf.at[slot],
            send_sem=send_sem.at[slot],
            recv_sem=recv_sem.at[slot],
            device_id=device,
            device_id_type=MESH,
        )

    to_partner, to_outer = send_z(0, 1, partner), send_z(3, 2, outer)

    @pl.when(has_outer)
    def _():
        halo.wait_recv()

    level_1a = dot_split(rows_1a, ybuf[0:3].reshape(6 * chunk, half), True)
    zbuf[3] = next_levels(level_1a)[1]

    @pl.when(has_outer)
    def _():
        to_outer.start()

    wait_best(2)
    merge(2, 2, None)
    columns_of(3)
    level_1 = level_1a + dot_split(rows_1b, ybuf[3], True)
    level_2, zbuf[0] = next_levels(level_1)
    to_partner.start()
    out_1[0] = level_1[0:chunk]
    out_1[1] = level_1[2 * chunk : 3 * chunk]
    out_2[0] = level_2[0:quarter]
    out_2[1] = level_2[chunk : chunk + quarter]
    to_partner.wait_recv()

    @pl.when(has_outer)
    def _():
        to_outer.wait_recv()

    level_3 = dot_split(rows_3, zbuf[0:3].reshape(3 * chunk, zbuf.shape[2]), True)
    out_3[0] = level_3[0 : quarter // 2]
    out_3[1] = level_3[chunk : chunk + quarter // 2]

    for copy in partner_sends + [to_partner]:
        copy.wait_send()

    @pl.when(has_outer)
    def _():
        halo.wait_send()
        to_outer.wait_send()


def write_out(*refs):
    count = len(refs) // 2
    semaphores = refs[-1]
    copies = [pltpu.make_async_copy(refs[n], refs[count + n], semaphores.at[n]) for n in range(count)]
    for copy in copies:
        copy.start()
    for copy in copies:
        copy.wait()


def body(red_band, nir_band, cloud_class, date_ordinal):
    dates, strip, width = red_band.shape
    own = strip // 2
    chunk = strip // 4
    whole = pl.BlockSpec(memory_space=pltpu.VMEM)
    anywhere = pl.BlockSpec(memory_space=pl.ANY)
    outs = [jax.ShapeDtypeStruct((own, width), jnp.int32)] * 3
    outs += [jax.ShapeDtypeStruct((2, own >> n, width >> n), jnp.float32) for n in range(1, LEVELS + 1)]
    kept = [pltpu.VMEM(out.shape, out.dtype) for out in outs]
    stream = pltpu.VMEM((4, dates, chunk, width), jnp.int32)
    results = pl.pallas_call(
        kernel,
        out_shape=kept,
        in_specs=[anywhere] * 4,
        out_specs=[whole] * 6,
        scratch_shapes=[
            stream,
            stream,
            stream,
            pltpu.VMEM((4, 3, chunk, width), jnp.int32),
            pltpu.VMEM((3, 3, chunk, width), jnp.int32),
            pltpu.VMEM((2 * chunk, width + 2 * LANES), jnp.float32),
            pltpu.VMEM((4, 2 * chunk, width // 2), jnp.float32),
            pltpu.VMEM((4 * chunk, width // 2 + 2 * LANES), jnp.float32),
            pltpu.VMEM((chunk, width // 4 + 2 * LANES), jnp.float32),
            pltpu.VMEM((4, chunk, width // 8), jnp.float32),
            pltpu.SMEM((dates,), jnp.int32),
            pltpu.SemaphoreType.DMA((4, PARTS, 3)),
            pltpu.SemaphoreType.DMA,
            pltpu.SemaphoreType.DMA((3 + 3 * PARTS,)),
            pltpu.SemaphoreType.DMA((3 + 3 * PARTS,)),
        ],
        compiler_params=pltpu.CompilerParams(collective_id=0, has_side_effects=True),
        name="composite",
    )(red_band, nir_band, cloud_class, date_ordinal)
    return pl.pallas_call(
        write_out,
        out_shape=outs,
        in_specs=[whole] * 6,
        out_specs=[anywhere] * 6,
        scratch_shapes=[pltpu.SemaphoreType.DMA((6,))],
        name="write_out",
    )(*[pltpu.with_memory_space_constraint(result, pltpu.VMEM) for result in results])


def solution(mesh):
    in_specs = (
        P("dates", ("tiles", "rows"), None),
        P("dates", ("tiles", "rows"), None),
        P("dates", ("tiles", "rows"), None),
        P(("tiles", "dates")),
    )
    out_specs = (
        P(("tiles", "rows", "dates"), None),
        P(("tiles", "rows", "dates"), None),
        P(("tiles", "rows", "dates"), None),
        P(None, ("tiles", "rows", "dates"), None),
        P(None, ("tiles", "rows", "dates"), None),
        P(None, ("tiles", "rows", "dates"), None),
    )
    return jax.shard_map(body, mesh=mesh, in_specs=in_specs, out_specs=out_specs, check_vma=False)
```

```python
import functools

import jax
import jax.numpy as jnp
from jax import lax
from jax.experimental import pallas as pl
from jax.experimental.pallas import tpu as pltpu
from jax.sharding import PartitionSpec as P

LEVELS = 3
LIMB_BITS = 15
LIMB_MASK = (1 << LIMB_BITS) - 1
FLAG = 1 << 30
SCALE_BAND = 2.0**-30
LANES = 128
WIDTH = 512
PARTS = 2
MESH = pl.DeviceIdType.MESH


def taps(distance):
    far = (distance == 0) | (distance == 5)
    mid = (distance == 1) | (distance == 4)
    near = (distance == 2) | (distance == 3)
    return jnp.where(near, 0.3125, jnp.where(mid, 0.15625, jnp.where(far, 0.03125, 0.0)))


def limbs(value):
    return value >> LIMB_BITS, value & LIMB_MASK


def take_first(first, second):
    r1a, r0a, n1a, n0a, clear_a, ord_a = first
    r1b, r0b, n1b, n0b, clear_b, ord_b = second
    low = n0a * r0b - n0b * r0a + ((ord_b - ord_a) >> 31)
    mid = (n1a * r0b + n0a * r1b) - (n1b * r0a + n0b * r1a) + (low >> LIMB_BITS)
    high = n1a * r1b - n1b * r1a + (mid >> LIMB_BITS)
    return high >= clear_b - clear_a


def pick(take, first, second):
    return tuple(jnp.where(take, one, two) for one, two in zip(first, second))


def joined(entry):
    r1, r0, n1, n0, clear, order = entry
    return (r1 << LIMB_BITS) | r0, (n1 << LIMB_BITS) | n0, clear, order


def dot_split(left, right, exact_left):
    data = right if exact_left else left
    high = data.astype(jnp.bfloat16)
    low = (data - high.astype(jnp.float32)).astype(jnp.bfloat16)
    if exact_left:
        dot = lambda part: jnp.dot(left, part, preferred_element_type=jnp.float32)
    else:
        dot = lambda part: jnp.dot(part, right, preferred_element_type=jnp.float32)
    return dot(high) + dot(low)


def filter_columns(source, weights):
    rows = source.shape[0]
    blocks = (source.shape[1] - 2 * LANES) // (2 * LANES)
    left = jnp.concatenate([source[:, 2 * LANES * b : 2 * LANES * b + 4 * LANES] for b in range(blocks)], axis=0)
    out = dot_split(left, weights, False)
    return [out[b * rows : (b + 1) * rows] for b in range(blocks)]


def iota(shape, axis):
    return lax.broadcasted_iota(jnp.int32, shape, axis)


def kernel(
    red, nir, cloud, ordinals, out_red, out_nir, out_ord, out_1, out_2, out_3,
    in_red, in_nir, in_cloud, best, arrived, wide_0, ybuf, wide_1, wide_2, zbuf,
    ords, load_sem, order_sem, send_sem, recv_sem,
):
    tile = lax.axis_index("tiles")
    strip_index = lax.axis_index("rows")
    core = lax.axis_index("dates")
    strips = lax.axis_size("rows")
    dates, strip, width = red.shape
    chunk = strip // 4
    half = width // 2
    has_outer = jnp.where(core == 0, strip_index > 0, strip_index < strips - 1)
    outer_strip = jnp.clip(strip_index + 2 * core - 1, 0, strips - 1)
    partner = (tile, strip_index, 1 - core)
    outer = (tile, outer_strip, 1 - core)
    rows_of = [(3 - 3 * core) * chunk, 3 * core * chunk, (2 - core) * chunk, (1 + core) * chunk]

    loads = []
    piece = width // PARTS
    for slot, begin in enumerate(rows_of):
        begin = pl.multiple_of(begin, chunk)
        for part in range(PARTS):
            columns = pl.ds(part * piece, piece)
            group = [
                pltpu.make_async_copy(
                    source.at[:, pl.ds(begin, chunk), columns],
                    target.at[slot, :, :, columns],
                    load_sem.at[slot, part, number],
                )
                for number, (source, target) in enumerate(((red, in_red), (nir, in_nir), (cloud, in_cloud)))
            ]
            for copy in group:
                copy.start()
            loads.append(group)
    order_copy = pltpu.make_async_copy(ordinals, ords, order_sem)
    order_copy.start()

    barrier = pltpu.get_barrier_semaphore()
    pl.semaphore_signal(barrier, inc=1, device_id=partner, device_id_type=MESH)

    @pl.when(has_outer)
    def _():
        pl.semaphore_signal(barrier, inc=1, device_id=outer, device_id_type=MESH)

    k = iota((4 * LANES, LANES), 0)
    j = iota((4 * LANES, LANES), 1)
    column_weights = taps(k - LANES - (2 * j - 2)).astype(jnp.bfloat16)

    @pl.when(jnp.logical_not(has_outer))
    def _():
        ybuf[2] = jnp.zeros(ybuf.shape[1:], jnp.float32)
        zbuf[2] = jnp.zeros(zbuf.shape[1:], jnp.float32)

    for wide in (wide_0, wide_1, wide_2):
        edge = jnp.zeros((wide.shape[0], LANES), jnp.float32)
        wide[:, 0:LANES] = edge
        wide[:, wide.shape[1] - LANES :] = edge

    order_copy.wait()

    def find_best(slot, part):
        for copy in loads[slot * PARTS + part]:
            copy.wait()

        def step(number, unused):
            columns = pl.ds(pl.multiple_of(number * WIDTH + part * piece, WIDTH), WIDTH)

            def entry(date):
                red_hi, red_lo = limbs(in_red[slot, date, :, columns])
                nir_hi, nir_lo = limbs(in_nir[slot, date, :, columns])
                clear = jnp.where(in_cloud[slot, date, :, columns] == 0, FLAG, 0)
                return (red_hi, red_lo, nir_hi, nir_lo, clear, ords[date])

            current = None
            for date in range(0, dates, 2):
                other = entry(date)
                if date + 1 < dates:
                    later = entry(date + 1)
                    other = pick(take_first(later, other), later, other)
                current = other if current is None else pick(take_first(other, current), other, current)
            value_red, value_nir, clear, order = joined(current)
            best[slot, 0, :, columns] = value_red
            best[slot, 1, :, columns] = value_nir
            best[slot, 2, :, columns] = clear + order
            return unused

        lax.fori_loop(0, piece // WIDTH, step, 0)

    partner_sends = []

    def send_best(slot, place, part):
        columns = pl.ds(part * piece, piece)
        copy = pltpu.make_async_remote_copy(
            src_ref=best.at[slot, :, :, columns],
            dst_ref=arrived.at[place, :, :, columns],
            send_sem=send_sem.at[3 + place * PARTS + part],
            recv_sem=recv_sem.at[3 + place * PARTS + part],
            device_id=partner,
            device_id_type=MESH,
        )
        copy.start()
        partner_sends.append(copy)

    def wait_best(place):
        for copy in partner_sends[place * PARTS : (place + 1) * PARTS]:
            copy.wait_recv()

    def merge(slot, place, out_row):
        def step(number, unused):
            at = pl.multiple_of(number * WIDTH, WIDTH)
            columns = pl.ds(at, WIDTH)

            def entry(source):
                red_hi, red_lo = limbs(source[0, :, columns])
                nir_hi, nir_lo = limbs(source[1, :, columns])
                packed = source[2, :, columns]
                return (red_hi, red_lo, nir_hi, nir_lo, packed & FLAG, packed & (FLAG - 1))

            mine, theirs = entry(best.at[slot]), entry(arrived.at[place])
            value_red, value_nir, clear, order = joined(pick(take_first(theirs, mine), theirs, mine))
            if out_row is not None:
                rows = pl.ds(pl.multiple_of(out_row, chunk), chunk)
                out_red[rows, columns] = value_red
                out_nir[rows, columns] = value_nir
                out_ord[rows, columns] = order
            inner = pl.ds(pl.multiple_of(at + LANES, LANES), WIDTH)
            wide_0[0:chunk, inner] = value_red.astype(jnp.float32) * SCALE_BAND
            wide_0[chunk : 2 * chunk, inner] = value_nir.astype(jnp.float32) * SCALE_BAND
            return unused

        lax.fori_loop(0, width // WIDTH, step, 0)

    def columns_of(place):
        for number, block in enumerate(filter_columns(wide_0, column_weights)):
            ybuf[place, :, number * LANES : (number + 1) * LANES] = block

    for part in range(PARTS):
        find_best(0, part)
        if part == 0:
            pl.semaphore_wait(barrier, 1 + has_outer.astype(jnp.int32))
        send_best(0, 0, part)
    for part in range(PARTS):
        find_best(1, part)
    wait_best(0)
    merge(1, 0, core * chunk)
    columns_of(0)
    halo = pltpu.make_async_remote_copy(
        src_ref=ybuf.at[0],
        dst_ref=ybuf.at[2],
        send_sem=send_sem.at[0],
        recv_sem=recv_sem.at[0],
        device_id=outer,
        device_id_type=MESH,
    )

    @pl.when(has_outer)
    def _():
        halo.start()

    for slot, place in ((2, 1), (3, 2)):
        for part in range(PARTS):
            find_best(slot, part)
            send_best(slot, place, part)
    wait_best(1)
    merge(3, 1, (1 - core) * chunk)
    columns_of(1)

    quarter = chunk // 2
    def row_weights(first, count):
        shape = (4 * chunk, count * 2 * chunk)
        m = iota(shape, 0)
        band_m = m // (2 * chunk)
        within = m % (2 * chunk)
        row_1 = jnp.where(within < chunk, within, jnp.where(within < chunk + quarter, within - chunk - quarter, within - quarter))
        c = iota(shape, 1)
        place = c // (2 * chunk) + first
        band_c = (c // chunk) % 2
        from_core_0 = jnp.where(place == 2, -chunk, jnp.where(place == 3, 2 * chunk, place * chunk))
        from_core_1 = chunk - from_core_0
        row_0 = jnp.where(core == 0, from_core_0, from_core_1) + c % chunk
        from_edge = jnp.where(core == 0, row_1, chunk - 1 - row_1)
        inside = from_edge >= jnp.where(has_outer, -chunk, 0)
        return jnp.where((band_m == band_c) & inside, taps(row_0 - (2 * row_1 - 2)), 0.0).astype(jnp.bfloat16)

    rows_1a, rows_1b = row_weights(0, 3), row_weights(3, 1)

    m = iota((3 * chunk, 4 * chunk), 0)
    packed = m >= 2 * chunk
    band_m = jnp.where(packed, (m - 2 * chunk) // quarter, m // chunk)
    row_2 = jnp.where(packed, m % quarter, m % chunk)
    c = iota((3 * chunk, 4 * chunk), 1)
    band_c = c // (2 * chunk)
    within = c % (2 * chunk)
    row_1 = jnp.where(within < chunk, within, jnp.where(within < chunk + quarter, within - chunk - quarter, within - quarter))
    rows_2 = jnp.where(band_m == band_c, taps(row_1 - (2 * row_2 - 2)), 0.0).astype(jnp.bfloat16)

    m = iota((2 * chunk, 3 * chunk), 0)
    c = iota((2 * chunk, 3 * chunk), 1)
    place = c // chunk
    toward = quarter * (1 - 2 * core)
    side = jnp.where(place == 0, 0, jnp.where(place == 1, toward, -toward))
    row_2 = c % quarter + side
    rows_3 = jnp.where(m // chunk == (c % chunk) // quarter, taps(row_2 - (2 * (m % chunk) - 2)), 0.0)
    rows_3 = rows_3.astype(jnp.bfloat16)

    def next_levels(level_1):
        wide_1[:, LANES : LANES + half] = level_1
        data = jnp.concatenate(filter_columns(wide_1, column_weights), axis=1)
        level_2 = dot_split(rows_2, data, True)
        wide_2[:, LANES : LANES + half // 2] = level_2[2 * chunk :]
        return level_2, jnp.concatenate(filter_columns(wide_2, column_weights), axis=1)

    def send_z(source, slot, device):
        return pltpu.make_async_remote_copy(
            src_ref=zbuf.at[source],
            dst_ref=zbuf.at[slot],
            send_sem=send_sem.at[slot],
            recv_sem=recv_sem.at[slot],
            device_id=device,
            device_id_type=MESH,
        )

    to_partner, to_outer = send_z(0, 1, partner), send_z(3, 2, outer)

    @pl.when(has_outer)
    def _():
        halo.wait_recv()

    level_1a = dot_split(rows_1a, ybuf[0:3].reshape(6 * chunk, half), True)
    zbuf[3] = next_levels(level_1a)[1]

    @pl.when(has_outer)
    def _():
        to_outer.start()

    wait_best(2)
    merge(2, 2, None)
    columns_of(3)
    level_1 = level_1a + dot_split(rows_1b, ybuf[3], True)
    level_2, zbuf[0] = next_levels(level_1)
    to_partner.start()
    out_1[0] = level_1[0:chunk]
    out_1[1] = level_1[2 * chunk : 3 * chunk]
    out_2[0] = level_2[0:quarter]
    out_2[1] = level_2[chunk : chunk + quarter]
    to_partner.wait_recv()

    @pl.when(has_outer)
    def _():
        to_outer.wait_recv()

    level_3 = dot_split(rows_3, zbuf[0:3].reshape(3 * chunk, zbuf.shape[2]), True)
    out_3[0] = level_3[0 : quarter // 2]
    out_3[1] = level_3[chunk : chunk + quarter // 2]

    for copy in partner_sends + [to_partner]:
        copy.wait_send()

    @pl.when(has_outer)
    def _():
        halo.wait_send()
        to_outer.wait_send()


def write_out(*refs):
    count = len(refs) // 2
    semaphores = refs[-1]
    copies = [pltpu.make_async_copy(refs[n], refs[count + n], semaphores.at[n]) for n in range(count)]
    for copy in copies:
        copy.start()
    for copy in copies:
        copy.wait()


def body(red_band, nir_band, cloud_class, date_ordinal):
    dates, strip, width = red_band.shape
    own = strip // 2
    chunk = strip // 4
    whole = pl.BlockSpec(memory_space=pltpu.VMEM)
    anywhere = pl.BlockSpec(memory_space=pl.ANY)
    outs = [jax.ShapeDtypeStruct((own, width), jnp.int32)] * 3
    outs += [jax.ShapeDtypeStruct((2, own >> n, width >> n), jnp.float32) for n in range(1, LEVELS + 1)]
    kept = [pltpu.VMEM(out.shape, out.dtype) for out in outs]
    stream = pltpu.VMEM((4, dates, chunk, width), jnp.int32)
    results = pl.pallas_call(
        kernel,
        out_shape=kept,
        in_specs=[anywhere] * 4,
        out_specs=[whole] * 6,
        scratch_shapes=[
            stream,
            stream,
            stream,
            pltpu.VMEM((4, 3, chunk, width), jnp.int32),
            pltpu.VMEM((3, 3, chunk, width), jnp.int32),
            pltpu.VMEM((2 * chunk, width + 2 * LANES), jnp.float32),
            pltpu.VMEM((4, 2 * chunk, width // 2), jnp.float32),
            pltpu.VMEM((4 * chunk, width // 2 + 2 * LANES), jnp.float32),
            pltpu.VMEM((chunk, width // 4 + 2 * LANES), jnp.float32),
            pltpu.VMEM((4, chunk, width // 8), jnp.float32),
            pltpu.SMEM((dates,), jnp.int32),
            pltpu.SemaphoreType.DMA((4, PARTS, 3)),
            pltpu.SemaphoreType.DMA,
            pltpu.SemaphoreType.DMA((3 + 3 * PARTS,)),
            pltpu.SemaphoreType.DMA((3 + 3 * PARTS,)),
        ],
        compiler_params=pltpu.CompilerParams(collective_id=0, has_side_effects=True),
        name="composite",
    )(red_band, nir_band, cloud_class, date_ordinal)
    return pl.pallas_call(
        write_out,
        out_shape=outs,
        in_specs=[whole] * 6,
        out_specs=[anywhere] * 6,
        scratch_shapes=[pltpu.SemaphoreType.DMA((6,))],
        name="write_out",
    )(*[pltpu.with_memory_space_constraint(result, pltpu.VMEM) for result in results])


def solution(mesh):
    in_specs = (
        P("dates", ("tiles", "rows"), None),
        P("dates", ("tiles", "rows"), None),
        P("dates", ("tiles", "rows"), None),
        P(("tiles", "dates")),
    )
    out_specs = (
        P(("tiles", "rows", "dates"), None),
        P(("tiles", "rows", "dates"), None),
        P(("tiles", "rows", "dates"), None),
        P(None, ("tiles", "rows", "dates"), None),
        P(None, ("tiles", "rows", "dates"), None),
        P(None, ("tiles", "rows", "dates"), None),
    )
    return jax.shard_map(body, mesh=mesh, in_specs=in_specs, out_specs=out_specs, check_vma=False)
```
